32 devices in a mesh: dom: 8 (over y, x, core), sub: 4 (over z).
Axes of the slice: x: 2, y: 2, z: 4, core: 2. Of those that a mesh axis runs over, the one named last changes fastest.
Arguments:
- features: bfloat16 [32768, 602], P(('dom', 'sub')), may hold values from -6 to 6
- w_inner: bfloat16 [602, 256], replicated, may hold values from -0.25 to 0.25
- bias_inner: float32 [256], replicated, may hold values from -6 to 6
- w_outer: bfloat16 [256, 41], replicated, may hold values from -0.375 to 0.375
- bias_outer: float32 [41], replicated, may hold values from -6 to 6
- tiles: bfloat16 [256, 32, 128, 128], P(('dom', 'sub')), may hold values from -3 to 3
- tile_col: int32 [256, 32], P(('dom', 'sub')), may hold values from 0 to 39, as said below
- degrees: int32 [32768], P(('dom', 'sub')), may hold values from 1 to 32
- send_rows: int32 [32, 32, 128], P(('dom', 'sub')), may hold values from -1 to 1023, as said below
Outputs:
- logits: float32 [32768, 41], P(('dom', 'sub'))
The draws below stay inside these ranges and needn't reach their ends.
Inputs may be any that keep to these rules, and one draw needn't show every extreme that they name: send_rows[e, p, s] is the row, among device e's 1024 vertices, that fills slot s of e's list for device p, or -1 for an unused slot; live slots come first and every list has 1 to 128 live slots; every sender has a full list, and in every draw some device receives full lists from all senders. tile_col[d * 8 + r, t] is the column block, in device d's column space, of tile t of row block r; the 32 column blocks of a row block are distinct.
All inputs are finite; a program needn't handle non-finite values.
Results may differ from the reference program's by a relative error of at most 0.0042.
Values may be sent and summed in bfloat16 or wider, within the bound.
No kernel may reach another device: no remote copies, remote signals or barrier semaphores. Data moves between devices by JAX's collectives and lax.ppermute only.
A program may use at most 128 MiB of HBM per device.

```python
import jax
import jax.numpy as jnp
from jax import lax

F_IN = 602
HID = 256
CLASSES = 41
BLK = 128
TILES = 32
V_DEV = 1024
PEERS = 32
ROW_BLOCKS = 8
COL_BLOCKS = 40
VERTS = 32768


def draw_send_rows(key, part):
    key_rows = jax.random.fold_in(key, 11)
    key_counts = jax.random.fold_in(key, 12)
    key_full = jax.random.fold_in(key, 13)
    key_target = jax.random.fold_in(key, 14)
    picked = jax.random.randint(key_rows, (PEERS, PEERS, BLK), 0, V_DEV)
    counts = jax.random.randint(key_counts, (PEERS, PEERS), 1, BLK + 1)
    full_peer = jax.random.randint(key_full, (PEERS,), 0, PEERS)
    target = jax.random.randint(key_target, (), 0, PEERS)
    peer_ids = jnp.arange(PEERS)
    counts = jnp.where(peer_ids[None, :] == full_peer[:, None], BLK, counts)
    counts = jnp.where(peer_ids[None, :] == target, BLK, counts)
    slots = jnp.arange(BLK)
    return jnp.where(slots[None, None, :] < counts[:, :, None], picked, -1).astype(jnp.int32)


def draw_tile_col(key, part):
    keys = jax.random.split(jax.random.fold_in(key, 21), PEERS)
    orders = jax.vmap(lambda single: jax.random.permutation(single, COL_BLOCKS))(keys)
    flat = jnp.arange(ROW_BLOCKS * TILES) % COL_BLOCKS
    picked = orders[:, flat]
    return picked.reshape(PEERS * ROW_BLOCKS, TILES).astype(jnp.int32)


def place_ends(drawn, stream_key, least, top_value):
    index_at = [jax.random.randint(jax.random.fold_in(stream_key, axis), (), 0, length) for axis, length in enumerate(drawn.shape)]
    main_axis = drawn.shape.index(max(drawn.shape))
    beside = index_at[:main_axis] + [(index_at[main_axis] + 1) % drawn.shape[main_axis]] + index_at[main_axis + 1:]
    return drawn.at[tuple(index_at)].set(least).at[tuple(beside)].set(top_value)


def levels(rng, dims, shards, low, largest):
    def one(position, blocks):
        draws = jax.random.uniform(jax.random.fold_in(jax.random.fold_in(rng, 6), position), (blocks,), jnp.float32, low / len(shards), largest / len(shards))
        return jnp.repeat(jnp.exp(draws), dims[position] // blocks).reshape((-1,) + (1,) * (len(dims) - position - 1))

    gain = one(*shards[0])
    for cut in shards[1:]:
        gain = gain * one(*cut)
    return gain


def centred(stream_key, extent, scale, reach, cuts=(), kind=jnp.bfloat16):
    drawn = scale * jax.random.normal(stream_key, extent, jnp.float32)
    if cuts:
        drawn = drawn * levels(stream_key, extent, cuts, -0.22, 0.18)
    return jnp.clip(drawn, -reach, reach).astype(kind)


def setup_inputs(seed: int = 0) -> dict:
    key_of = jax.random.split(jax.random.key(seed), 10)
    return {
        "features": centred(key_of[0], (VERTS, F_IN), 1.0, 6.0, ((0, 32),)),
        "w_inner": centred(key_of[1], (F_IN, HID), F_IN ** -0.5, 0.25),
        "bias_inner": centred(key_of[2], (HID,), 1.0, 6.0, (), jnp.float32),
        "w_outer": centred(key_of[3], (HID, CLASSES), HID ** -0.5, 0.375),
        "bias_outer": centred(key_of[4], (CLASSES,), 1.0, 6.0, (), jnp.float32),
        "tiles": centred(key_of[5], (PEERS * ROW_BLOCKS, TILES, BLK, BLK), (12.0 / (TILES * BLK) ** 0.5), 3.0, ((0, 32),)),
        "tile_col": draw_tile_col(jax.random.fold_in(key_of[9], 71), 0),
        "degrees": place_ends(jax.random.randint(key_of[7], (VERTS,), 1, 33), jax.random.fold_in(key_of[7], 1), 1, 32).astype(jnp.int32),
        "send_rows": draw_send_rows(jax.random.fold_in(key_of[9], 71), 0),
    }


def aggregate(feature_rows, tiles, tile_col, send_rows):
    width = feature_rows.shape[1]
    by_device = feature_rows.reshape(PEERS, V_DEV, width)
    tile_sets = tiles.reshape(PEERS, ROW_BLOCKS, TILES, BLK, BLK)
    col_sets = tile_col.reshape(PEERS, ROW_BLOCKS, TILES)

    def per_target(target):
        slot_rows = lax.dynamic_index_in_dim(send_rows, target, 1, keepdims=False)
        clipped = jnp.clip(slot_rows, 0, V_DEV - 1).astype(jnp.int32)
        fetched = jnp.take_along_axis(by_device, clipped[:, :, None], axis=1)
        fetched = jnp.where((slot_rows >= 0)[:, :, None], fetched, jnp.zeros((), feature_rows.dtype))
        own_rows = lax.dynamic_index_in_dim(by_device, target, 0, keepdims=False)
        columns = jnp.concatenate([own_rows.reshape(ROW_BLOCKS, BLK, width), fetched], axis=0)
        target_tiles = lax.dynamic_index_in_dim(tile_sets, target, 0, keepdims=False)
        target_cols = lax.dynamic_index_in_dim(col_sets, target, 0, keepdims=False)
        blocks = columns[target_cols]
        summed = jnp.einsum('rtij,rtjw->riw', target_tiles.astype(jnp.float32), blocks.astype(jnp.float32))
        return summed.reshape(V_DEV, width)
    results = lax.map(per_target, jnp.arange(PEERS, dtype=jnp.int32))
    return results.reshape(PEERS * V_DEV, width)

def reference(features, w_inner, bias_inner, w_outer, bias_outer, tiles, tile_col, degrees, send_rows):
    inv_sqrt = lax.rsqrt(degrees.astype(jnp.float32))[:, None]
    projected = (jnp.dot(features, w_inner, preferred_element_type=jnp.float32) * inv_sqrt).astype(jnp.bfloat16)
    agg_inner = aggregate(projected, tiles, tile_col, send_rows)
    hidden = (inv_sqrt * jax.nn.relu(inv_sqrt * agg_inner + bias_inner)).astype(jnp.bfloat16)
    scores = jnp.dot(hidden, w_outer, preferred_element_type=jnp.float32).astype(jnp.bfloat16)
    agg_outer = aggregate(scores, tiles, tile_col, send_rows)
    return inv_sqrt * agg_outer + bias_outer
```

```python
import functools

import jax
import jax.numpy as jnp
from jax import lax
from jax.experimental import pallas as pl
from jax.experimental.pallas import tpu as pltpu
from jax.sharding import PartitionSpec as P

AXES = ("dom", "sub")
NT = (((1,), (1,)), ((), ()))
TN = (((0,), (0,)), ((), ()))
SMEM = pl.BlockSpec(memory_space=pltpu.SMEM)
VMEM = pl.BlockSpec(memory_space=pltpu.VMEM)
ANY = pl.BlockSpec(memory_space=pl.ANY)


def one_hot_rows(slots, rows):
    lane = lax.broadcasted_iota(jnp.int32, (slots.shape[0], rows), 1)
    return jnp.where(slots == lane, 1.0, 0.0).astype(jnp.bfloat16)


def one_hot_cols(slots, rows):
    sub = lax.broadcasted_iota(jnp.int32, (rows, slots.shape[1]), 0)
    return jnp.where(slots == sub, 1.0, 0.0).astype(jnp.bfloat16)


def inv_sqrt_columns(deg_ref):
    return jnp.transpose(lax.rsqrt(deg_ref[...].astype(jnp.float32)))


def project_kernel(feat_ref, w_ref, deg_ref, send_ref, proj_ref, out_ref):
    blocks, blk, _ = proj_ref.shape
    rows = blocks * blk

    @pl.when(pl.program_id(0) == 0)
    def _():
        inv = inv_sqrt_columns(deg_ref)
        for b in range(blocks):
            part = lax.dot_general(
                feat_ref[:, b * blk : (b + 1) * blk],
                w_ref[...],
                TN,
                preferred_element_type=jnp.float32,
            )
            proj_ref[b] = (part * inv[:, b : b + 1]).astype(proj_ref.dtype)

    slots = jnp.transpose(send_ref[...])
    table = proj_ref[...].reshape(rows, proj_ref.shape[2])
    for p in range(out_ref.shape[0]):
        picked = jnp.dot(
            one_hot_rows(slots[:, p : p + 1], rows), table, preferred_element_type=jnp.float32
        )
        out_ref[p] = picked.astype(out_ref.dtype)


def project_and_pick(feat_t, w_inner, deg, send_lists):
    f_in, rows = feat_t.shape
    hid = w_inner.shape[1]
    peers, blk = send_lists.shape
    blocks = rows // blk
    chunk = 8 if peers % 8 == 0 else peers
    return pl.pallas_call(
        project_kernel,
        grid=(peers // chunk,),
        in_specs=[
            pl.BlockSpec((f_in, rows), lambda g: (0, 0)),
            pl.BlockSpec((f_in, hid), lambda g: (0, 0)),
            pl.BlockSpec((blocks, blk), lambda g: (0, 0)),
            pl.BlockSpec((chunk, blk), lambda g: (g, 0)),
        ],
        out_specs=[
            pl.BlockSpec((blocks, blk, hid), lambda g: (0, 0, 0)),
            pl.BlockSpec((chunk, blk, hid), lambda g: (g, 0, 0)),
        ],
        out_shape=[
            jax.ShapeDtypeStruct((blocks, blk, hid), jnp.bfloat16),
            jax.ShapeDtypeStruct((peers, blk, hid), jnp.bfloat16),
        ],
        name="project_pick",
    )(feat_t, w_inner, deg, send_lists)


def start_fetches(own, arrived, tiles, columns, tiles_v, sems):
    own_blocks = own.shape[0]
    row_blocks = tiles.shape[0]
    first = pltpu.make_async_copy(own, columns.at[pl.ds(0, own_blocks)], sems.at[0])
    second = pltpu.make_async_copy(
        arrived, columns.at[pl.ds(own_blocks, arrived.shape[0])], sems.at[1]
    )
    sets = [
        pltpu.make_async_copy(tiles.at[r], tiles_v.at[r], sems.at[2 + r]) for r in range(row_blocks)
    ]
    for copy in [first, second] + sets:
        copy.start()

    def wait_columns():
        first.wait()
        second.wait()

    return wait_columns, [copy.wait for copy in sets]


def inner_kernel(
    col_ref, own, arrived, tiles, deg_ref, bias_ref, wt_ref, send_ref,
    scores_ref, out_ref, columns, tiles_v, table, sems,
):
    row_blocks, per_row, blk, _ = tiles.shape
    peers = send_ref.shape[0]
    rows = row_blocks * blk
    wait_columns, wait_tiles = start_fetches(own, arrived, tiles, columns, tiles_v, sems)
    inv = inv_sqrt_columns(deg_ref)
    wait_columns()
    for r in range(row_blocks):
        wait_tiles[r]()
        total = jnp.zeros((blk, columns.shape[2]), jnp.float32)
        for t in range(0, per_row, 2):
            left = jnp.concatenate([tiles_v[r, t], tiles_v[r, t + 1]], axis=1)
            right = jnp.concatenate([columns[col_ref[r, t]], columns[col_ref[r, t + 1]]], axis=0)
            total = total + jnp.dot(left, right, preferred_element_type=jnp.float32)
        scale = inv[:, r : r + 1]
        hidden = (scale * jax.nn.relu(scale * total + bias_ref[...])).astype(jnp.bfloat16)
        scores = lax.dot_general(wt_ref[...], hidden, NT, preferred_element_type=jnp.float32)
        scores = scores.astype(jnp.bfloat16)
        scores_ref[r] = scores
        table[:, r * blk : (r + 1) * blk] = scores

    def pick(step, carry):
        base = step * 4
        for half in range(2):
            p = base + 2 * half
            slots = jnp.concatenate([send_ref[pl.ds(p, 1)], send_ref[pl.ds(p + 1, 1)]], axis=1)
            picked = jnp.dot(
                table[...], one_hot_cols(slots, rows), preferred_element_type=jnp.float32
            ).astype(out_ref.dtype)
            out_ref[p] = picked[:, :blk]
            out_ref[p + 1] = picked[:, blk:]
        return carry

    lax.fori_loop(0, peers // 4, pick, 0)


def aggregate_inner(tile_col, own, arrived, tiles, deg, bias, w_t, send_lists):
    classes = w_t.shape[0]
    blocks, blk, hid = own.shape
    peers = arrived.shape[0]
    return pl.pallas_call(
        inner_kernel,
        in_specs=[SMEM, ANY, ANY, ANY, VMEM, VMEM, VMEM, VMEM],
        out_specs=[VMEM, VMEM],
        out_shape=[
            jax.ShapeDtypeStruct((blocks, classes, blk), jnp.bfloat16),
            jax.ShapeDtypeStruct((peers, classes, blk), jnp.bfloat16),
        ],
        scratch_shapes=[
            pltpu.VMEM((blocks + peers, blk, hid), jnp.bfloat16),
            pltpu.VMEM(tiles.shape, jnp.bfloat16),
            pltpu.VMEM((classes, blocks * blk), jnp.bfloat16),
            pltpu.SemaphoreType.DMA((2 + blocks,)),
        ],
        name="aggregate_inner",
    )(tile_col, own, arrived, tiles, deg, bias, w_t, send_lists)


def outer_kernel(
    col_ref, own, arrived, tiles, deg_ref, bias_ref, out_ref, columns, tiles_v, sems
):
    row_blocks, per_row, blk, _ = tiles.shape
    classes = out_ref.shape[0]
    wait_columns, wait_tiles = start_fetches(own, arrived, tiles, columns, tiles_v, sems)
    inv = lax.rsqrt(deg_ref[...].astype(jnp.float32))
    square = (classes, classes)
    diagonal = lax.broadcasted_iota(jnp.int32, square, 0) == lax.broadcasted_iota(jnp.int32, square, 1)
    bias = jnp.sum(jnp.where(diagonal, bias_ref[...], 0.0), axis=1, keepdims=True)
    wait_columns()
    for r in range(row_blocks):
        wait_tiles[r]()
        total = jnp.zeros((classes, blk), jnp.float32)
        for t in range(0, per_row, 2):
            left = jnp.concatenate([columns[col_ref[r, t]], columns[col_ref[r, t + 1]]], axis=1)
            right = jnp.concatenate([tiles_v[r, t], tiles_v[r, t + 1]], axis=1)
            total = total + lax.dot_general(left, right, NT, preferred_element_type=jnp.float32)
        out_ref[:, r * blk : (r + 1) * blk] = inv[r : r + 1] * total + bias


def aggregate_outer(tile_col, own, arrived, tiles, deg, bias):
    blocks, classes, blk = own.shape
    peers = arrived.shape[0]
    return pl.pallas_call(
        outer_kernel,
        in_specs=[SMEM, ANY, ANY, ANY, VMEM, VMEM],
        out_specs=VMEM,
        out_shape=jax.ShapeDtypeStruct((classes, blocks * blk), jnp.float32),
        scratch_shapes=[
            pltpu.VMEM((blocks + peers, classes, blk), jnp.bfloat16),
            pltpu.VMEM(tiles.shape, jnp.bfloat16),
            pltpu.SemaphoreType.DMA((2 + blocks,)),
        ],
        name="aggregate_outer",
    )(tile_col, own, arrived, tiles, deg, bias)


def exchange(outgoing):
    return lax.all_to_all(outgoing, AXES, split_axis=0, concat_axis=0, tiled=True)


def on_device(
    features, w_inner, bias_inner, w_outer, bias_outer, tiles, tile_col, degrees, send_rows
):
    send_lists = send_rows[0]
    deg = degrees.reshape(-1, tiles.shape[2])
    own, outgoing = project_and_pick(features.T, w_inner, deg, send_lists)
    arrived = exchange(outgoing)
    own_scores, outgoing = aggregate_inner(
        tile_col, own, arrived, tiles, deg, bias_inner[None], w_outer.T, send_lists
    )
    arrived = exchange(outgoing)
    return aggregate_outer(tile_col, own_scores, arrived, tiles, deg, bias_outer[None]).T


def solution(mesh):
    return jax.shard_map(
        on_device,
        mesh=mesh,
        in_specs=(
            P(AXES, None),
            P(),
            P(),
            P(),
            P(),
            P(AXES, None, None, None),
            P(AXES, None),
            P(AXES),
            P(AXES, None, None),
        ),
        out_specs=P(AXES, None),
        check_vma=False,
    )
```

```python
import functools

import jax
import jax.numpy as jnp
from jax import lax
from jax.experimental import pallas as pl
from jax.experimental.pallas import tpu as pltpu
from jax.sharding import PartitionSpec as P

AXES = ("dom", "sub")
NT = (((1,), (1,)), ((), ()))
TN = (((0,), (0,)), ((), ()))
SMEM = pl.BlockSpec(memory_space=pltpu.SMEM)
VMEM = pl.BlockSpec(memory_space=pltpu.VMEM)
ANY = pl.BlockSpec(memory_space=pl.ANY)


def one_hot_rows(slots, rows):
    lane = lax.broadcasted_iota(jnp.int32, (slots.shape[0], rows), 1)
    return jnp.where(slots == lane, 1.0, 0.0).astype(jnp.bfloat16)


def one_hot_cols(slots, rows):
    sub = lax.broadcasted_iota(jnp.int32, (rows, slots.shape[1]), 0)
    return jnp.where(slots == sub, 1.0, 0.0).astype(jnp.bfloat16)


def inv_sqrt_columns(deg_ref):
    return jnp.transpose(lax.rsqrt(deg_ref[...].astype(jnp.float32)))


def project_kernel(feat_ref, w_ref, deg_ref, send_ref, proj_ref, out_ref):
    blocks, blk, _ = proj_ref.shape
    rows = blocks * blk

    @pl.when(pl.program_id(0) == 0)
    def _():
        inv = inv_sqrt_columns(deg_ref)
        for b in range(blocks):
            part = lax.dot_general(
                feat_ref[:, b * blk : (b + 1) * blk],
                w_ref[...],
                TN,
                preferred_element_type=jnp.float32,
            )
            proj_ref[b] = (part * inv[:, b : b + 1]).astype(proj_ref.dtype)

    slots = jnp.transpose(send_ref[...])
    table = proj_ref[...].reshape(rows, proj_ref.shape[2])
    for p in range(out_ref.shape[0]):
        picked = jnp.dot(
            one_hot_rows(slots[:, p : p + 1], rows), table, preferred_element_type=jnp.float32
        )
        out_ref[p] = picked.astype(out_ref.dtype)


def project_and_pick(feat_t, w_inner, deg, send_lists):
    f_in, rows = feat_t.shape
    hid = w_inner.shape[1]
    peers, blk = send_lists.shape
    blocks = rows // blk
    chunk = 8 if peers % 8 == 0 else peers
    return pl.pallas_call(
        project_kernel,
        grid=(peers // chunk,),
        in_specs=[
            pl.BlockSpec((f_in, rows), lambda g: (0, 0)),
            pl.BlockSpec((f_in, hid), lambda g: (0, 0)),
            pl.BlockSpec((blocks, blk), lambda g: (0, 0)),
            pl.BlockSpec((chunk, blk), lambda g: (g, 0)),
        ],
        out_specs=[
            pl.BlockSpec((blocks, blk, hid), lambda g: (0, 0, 0)),
            pl.BlockSpec((chunk, blk, hid), lambda g: (g, 0, 0)),
        ],
        out_shape=[
            jax.ShapeDtypeStruct((blocks, blk, hid), jnp.bfloat16),
            jax.ShapeDtypeStruct((peers, blk, hid), jnp.bfloat16),
        ],
        name="project_pick",
    )(feat_t, w_inner, deg, send_lists)


def start_fetches(own, arrived, tiles, columns, tiles_v, sems):
    own_blocks = own.shape[0]
    row_blocks = tiles.shape[0]
    first = pltpu.make_async_copy(own, columns.at[pl.ds(0, own_blocks)], sems.at[0])
    second = pltpu.make_async_copy(
        arrived, columns.at[pl.ds(own_blocks, arrived.shape[0])], sems.at[1]
    )
    sets = [
        pltpu.make_async_copy(tiles.at[r], tiles_v.at[r], sems.at[2 + r]) for r in range(row_blocks)
    ]
    for copy in [first, second] + sets:
        copy.start()

    def wait_columns():
        first.wait()
        second.wait()

    return wait_columns, [copy.wait for copy in sets]


def row_block_sum(tiles_v, columns, col_ref, r, product):
    total = None
    for t in range(0, tiles_v.shape[1], 2):
        left = jnp.concatenate([tiles_v[r, t], tiles_v[r, t + 1]], axis=1)
        part = product(left, columns[col_ref[r, t]], columns[col_ref[r, t + 1]])
        total = part if total is None else total + part
    return total


def row_blocks_in_pairs(row_blocks, wait_tiles, block_sum, finish):
    ready = []
    for first in range(0, row_blocks, 2):
        pair = range(first, min(first + 2, row_blocks))
        for r in pair:
            wait_tiles[r]()
        sums = [(r, block_sum(r)) for r in pair]
        for done in ready:
            finish(*done)
        ready = sums
    for done in ready:
        finish(*done)


def inner_kernel(
    col_ref, own, arrived, tiles, deg_ref, bias_ref, wt_ref, send_ref,
    scores_ref, out_ref, columns, tiles_v, table, sems,
):
    row_blocks, per_row, blk, _ = tiles.shape
    peers = send_ref.shape[0]
    rows = row_blocks * blk
    wait_columns, wait_tiles = start_fetches(own, arrived, tiles, columns, tiles_v, sems)
    inv = inv_sqrt_columns(deg_ref)

    def finish(r, total):
        scale = inv[:, r : r + 1]
        hidden = (scale * jax.nn.relu(scale * total + bias_ref[...])).astype(jnp.bfloat16)
        scores = lax.dot_general(wt_ref[...], hidden, NT, preferred_element_type=jnp.float32)
        scores = scores.astype(jnp.bfloat16)
        scores_ref[r] = scores
        table[:, r * blk : (r + 1) * blk] = scores

    def block_sum(r):
        return row_block_sum(
            tiles_v, columns, col_ref, r, lambda left, a, b: jnp.dot(
                left, jnp.concatenate([a, b], axis=0), preferred_element_type=jnp.float32
            )
        )

    wait_columns()
    row_blocks_in_pairs(row_blocks, wait_tiles, block_sum, finish)

    def pick(step, carry):
        base = step * 4
        for half in range(2):
            p = base + 2 * half
            slots = jnp.concatenate([send_ref[pl.ds(p, 1)], send_ref[pl.ds(p + 1, 1)]], axis=1)
            picked = jnp.dot(
                table[...], one_hot_cols(slots, rows), preferred_element_type=jnp.float32
            ).astype(out_ref.dtype)
            out_ref[p] = picked[:, :blk]
            out_ref[p + 1] = picked[:, blk:]
        return carry

    lax.fori_loop(0, peers // 4, pick, 0)


def aggregate_inner(tile_col, own, arrived, tiles, deg, bias, w_t, send_lists):
    classes = w_t.shape[0]
    blocks, blk, hid = own.shape
    peers = arrived.shape[0]
    return pl.pallas_call(
        inner_kernel,
        in_specs=[SMEM, ANY, ANY, ANY, VMEM, VMEM, VMEM, VMEM],
        out_specs=[VMEM, VMEM],
        out_shape=[
            jax.ShapeDtypeStruct((blocks, classes, blk), jnp.bfloat16),
            jax.ShapeDtypeStruct((peers, classes, blk), jnp.bfloat16),
        ],
        scratch_shapes=[
            pltpu.VMEM((blocks + peers, blk, hid), jnp.bfloat16),
            pltpu.VMEM(tiles.shape, jnp.bfloat16),
            pltpu.VMEM((classes, blocks * blk), jnp.bfloat16),
            pltpu.SemaphoreType.DMA((2 + blocks,)),
        ],
        name="aggregate_inner",
    )(tile_col, own, arrived, tiles, deg, bias, w_t, send_lists)


def outer_kernel(
    col_ref, own, arrived, tiles, deg_ref, bias_ref, out_ref, columns, tiles_v, sems
):
    row_blocks, per_row, blk, _ = tiles.shape
    classes = out_ref.shape[0]
    wait_columns, wait_tiles = start_fetches(own, arrived, tiles, columns, tiles_v, sems)
    inv = lax.rsqrt(deg_ref[...].astype(jnp.float32))
    square = (classes, classes)
    diagonal = lax.broadcasted_iota(jnp.int32, square, 0) == lax.broadcasted_iota(jnp.int32, square, 1)
    bias = jnp.sum(jnp.where(diagonal, bias_ref[...], 0.0), axis=1, keepdims=True)
    def block_sum(r):
        return row_block_sum(
            tiles_v, columns, col_ref, r, lambda left, a, b: lax.dot_general(
                left, jnp.concatenate([a, b], axis=1), NT, preferred_element_type=jnp.float32
            )
        )

    def finish(r, total):
        out_ref[:, r * blk : (r + 1) * blk] = inv[r : r + 1] * jnp.transpose(total) + bias

    wait_columns()
    row_blocks_in_pairs(row_blocks, wait_tiles, block_sum, finish)


def aggregate_outer(tile_col, own, arrived, tiles, deg, bias):
    blocks, classes, blk = own.shape
    peers = arrived.shape[0]
    return pl.pallas_call(
        outer_kernel,
        in_specs=[SMEM, ANY, ANY, ANY, VMEM, VMEM],
        out_specs=VMEM,
        out_shape=jax.ShapeDtypeStruct((classes, blocks * blk), jnp.float32),
        scratch_shapes=[
            pltpu.VMEM((blocks + peers, classes, blk), jnp.bfloat16),
            pltpu.VMEM(tiles.shape, jnp.bfloat16),
            pltpu.SemaphoreType.DMA((2 + blocks,)),
        ],
        name="aggregate_outer",
    )(tile_col, own, arrived, tiles, deg, bias)


def exchange(outgoing):
    return lax.all_to_all(outgoing, AXES, split_axis=0, concat_axis=0, tiled=True)


def on_device(
    features, w_inner, bias_inner, w_outer, bias_outer, tiles, tile_col, degrees, send_rows
):
    send_lists = send_rows[0]
    deg = degrees.reshape(-1, tiles.shape[2])
    own, outgoing = project_and_pick(features.T, w_inner, deg, send_lists)
    arrived = exchange(outgoing)
    own_scores, outgoing = aggregate_inner(
        tile_col, own, arrived, tiles, deg, bias_inner[None], w_outer.T, send_lists
    )
    arrived = exchange(outgoing)
    return aggregate_outer(tile_col, own_scores, arrived, tiles, deg, bias_outer[None]).T


def solution(mesh):
    return jax.shard_map(
        on_device,
        mesh=mesh,
        in_specs=(
            P(AXES, None),
            P(),
            P(),
            P(),
            P(),
            P(AXES, None, None, None),
            P(AXES, None),
            P(AXES),
            P(AXES, None, None),
        ),
        out_specs=P(AXES, None),
        check_vma=False,
    )
```

```python
import functools

import jax
import jax.numpy as jnp
from jax import lax
from jax.experimental import pallas as pl
from jax.experimental.pallas import tpu as pltpu
from jax.sharding import Mesh
from jax.sharding import PartitionSpec as P

NT = (((1,), (1,)), ((), ()))
TN = (((0,), (0,)), ((), ()))
SMEM = pl.BlockSpec(memory_space=pltpu.SMEM)
VMEM = pl.BlockSpec(memory_space=pltpu.VMEM)
ANY = pl.BlockSpec(memory_space=pl.ANY)
HBM = pl.BlockSpec(memory_space=pltpu.HBM)
ROOMY = pltpu.CompilerParams(vmem_limit_bytes=58 * 2**20)
SMALL = pltpu.CompilerParams(vmem_limit_bytes=24 * 2**20)
LIST_BITS = 5
RIGHT_BLOCKS = 5


def one_hot_rows(slots, rows):
    lane = lax.broadcasted_iota(jnp.int32, (slots.shape[0], rows), 1)
    return jnp.where(slots == lane, 1.0, 0.0).astype(jnp.bfloat16)


def one_hot_cols(slots, rows):
    sub = lax.broadcasted_iota(jnp.int32, (rows, slots.shape[1]), 0)
    return jnp.where(slots == sub, 1.0, 0.0).astype(jnp.bfloat16)


def inv_sqrt_columns(deg_ref):
    return jnp.transpose(lax.rsqrt(deg_ref[...].astype(jnp.float32)))


def half_lists(send_ref, side, groups):
    run = send_ref.shape[0] // (2 * groups)
    runs = []
    for g in range(groups):
        low = send_ref[2 * g * run : (2 * g + 1) * run]
        high = send_ref[(2 * g + 1) * run : (2 * g + 2) * run]
        runs.append(jnp.where(side == 0, low, high))
    return jnp.concatenate(runs, axis=0)


def project_kernel(
    side_ref, feat_ref, w_ref, deg_ref, send_ref, left_ref, right_ref, slots_ref, *, groups
):
    blocks, blk = deg_ref.shape
    left_rows = blocks * blk - right_ref.shape[0]
    inv = inv_sqrt_columns(deg_ref)
    for b in range(blocks):
        part = lax.dot_general(
            feat_ref[:, b * blk : (b + 1) * blk],
            w_ref[...],
            TN,
            preferred_element_type=jnp.float32,
        )
        part = (part * inv[:, b : b + 1]).astype(left_ref.dtype)
        if b * blk < left_rows:
            left_ref[b * blk : (b + 1) * blk, :] = part
        else:
            right_ref[b * blk - left_rows : (b + 1) * blk - left_rows, :] = part
    side = side_ref[0]
    lists = half_lists(send_ref, 1 - side, groups)
    coded = jnp.concatenate([lists >> LIST_BITS, lists & (2**LIST_BITS - 1)], axis=1)
    left_ref[left_rows:, :] = coded.astype(jnp.float32).astype(left_ref.dtype)
    slots_ref[...] = jnp.transpose(half_lists(send_ref, side, groups))


def project(side, feat_t, w_inner, deg, send_lists, right_blocks, groups):
    hid = w_inner.shape[1]
    blocks, blk = deg.shape
    lists = send_lists.shape[0] // 2
    left_rows = (blocks - right_blocks) * blk
    return pl.pallas_call(
        functools.partial(project_kernel, groups=groups),
        in_specs=[SMEM, VMEM, VMEM, VMEM, VMEM],
        out_specs=[VMEM] * 3,
        out_shape=[
            jax.ShapeDtypeStruct((left_rows + lists, hid), jnp.bfloat16),
            jax.ShapeDtypeStruct((right_blocks * blk, hid), jnp.bfloat16),
            jax.ShapeDtypeStruct((blk, lists), jnp.int32),
        ],
        name="project",
    )(side, feat_t, w_inner, deg, send_lists)


def pick_rows(slots, table, first):
    chosen = one_hot_rows(slots - first, table.shape[0])
    return jnp.dot(chosen, table, preferred_element_type=jnp.float32)


def pick_near_kernel(left_ref, right_ref, slots_ref, out_ref):
    lists = out_ref.shape[0]
    left_rows = left_ref.shape[0] - lists
    for p in range(lists):
        column = slots_ref[:, p : p + 1]
        picked = pick_rows(column, left_ref[:left_rows], 0)
        picked = picked + pick_rows(column, right_ref[...], left_rows)
        out_ref[p] = picked.astype(out_ref.dtype)


def pick_near(left, right, slots):
    blk, lists = slots.shape
    return pl.pallas_call(
        pick_near_kernel,
        in_specs=[VMEM, VMEM, VMEM],
        out_specs=VMEM,
        out_shape=jax.ShapeDtypeStruct((lists, blk, left.shape[1]), jnp.bfloat16),
        name="pick_near",
    )(left, right, slots)


def pick_left_kernel(left_ref, out_ref, slots_ref):
    lists, blk, _ = out_ref.shape
    left_rows = left_ref.shape[0] - lists
    coded = left_ref[left_rows:].astype(jnp.float32)
    whole = coded[:, :blk] * 2.0**LIST_BITS + coded[:, blk : 2 * blk]
    slots = jnp.transpose(whole).astype(jnp.int32)
    slots_ref[...] = slots
    for p in range(lists):
        picked = pick_rows(slots[:, p : p + 1], left_ref[:left_rows], 0)
        out_ref[p] = picked.astype(out_ref.dtype)


def pick_left(left, lists, blk):
    return pl.pallas_call(
        pick_left_kernel,
        in_specs=[VMEM],
        out_specs=[VMEM, VMEM],
        out_shape=[
            jax.ShapeDtypeStruct((lists, blk, left.shape[1]), jnp.bfloat16),
            jax.ShapeDtypeStruct((blk, lists), jnp.int32),
        ],
        compiler_params=SMALL,
        name="pick_left",
    )(left)


def pick_right_kernel(part_ref, slots_ref, right_ref, out_ref, *, left_rows):
    for p in range(out_ref.shape[0]):
        picked = pick_rows(slots_ref[:, p : p + 1], right_ref[...], left_rows)
        out_ref[p] = (part_ref[p].astype(jnp.float32) + picked).astype(out_ref.dtype)


def pick_right(part, slots, right, left_rows):
    return pl.pallas_call(
        functools.partial(pick_right_kernel, left_rows=left_rows),
        in_specs=[VMEM, VMEM, VMEM],
        out_specs=VMEM,
        out_shape=jax.ShapeDtypeStruct(part.shape, part.dtype),
        compiler_params=SMALL,
        name="pick_right",
    )(part, slots, right)


def start_fetches(column_copies, tiles, tiles_v, sems):
    row_blocks = tiles.shape[0]
    firsts = [
        pltpu.make_async_copy(src, dst, sems.at[row_blocks + i])
        for i, (src, dst) in enumerate(column_copies)
    ]
    sets = [
        pltpu.make_async_copy(tiles.at[r], tiles_v.at[r], sems.at[r]) for r in range(row_blocks)
    ]
    for copy in firsts + sets:
        copy.start()

    def wait_columns():
        for copy in firsts:
            copy.wait()

    def wait_pair(first):
        for copy in sets[first : first + 2]:
            copy.wait()

    return wait_columns, wait_pair


def row_block_sum(tiles_v, columns, col_ref, r, product):
    total = None
    for t in range(0, tiles_v.shape[1], 2):
        left = jnp.concatenate([tiles_v[r, t], tiles_v[r, t + 1]], axis=1)
        part = product(left, columns[col_ref[r, t]], columns[col_ref[r, t + 1]])
        total = part if total is None else total + part
    return total


def row_blocks_in_pairs(row_blocks, wait_pair, block_sum, finish):
    ready = []
    for first in range(0, row_blocks, 2):
        wait_pair(first)
        sums = [(r, block_sum(r)) for r in range(first, min(first + 2, row_blocks))]
        for done in ready:
            finish(*done)
        ready = sums
    for done in ready:
        finish(*done)


def inner_kernel(
    col_ref, side_ref, left, right, near, far, tiles, deg_ref, bias_ref, wt_ref,
    send_ref, scores_ref, out_ref, columns, tiles_v, table, sems, *, groups,
):
    row_blocks, _, blk, _ = tiles.shape
    peers = send_ref.shape[0]
    rows = row_blocks * blk
    run = near.shape[0] // groups
    side = side_ref[0]
    right_blocks = right.shape[0] // blk
    copies = []
    for b in range(row_blocks):
        late = b - (row_blocks - right_blocks)
        source, at = (left, b) if late < 0 else (right, late)
        copies.append((source.at[pl.ds(at * blk, blk)], columns.at[b]))
    for g in range(groups):
        base = row_blocks + 2 * g * run
        group = pl.ds(g * run, run)
        copies.append((near.at[group], columns.at[pl.ds(base + side * run, run)]))
        copies.append((far.at[group], columns.at[pl.ds(base + (1 - side) * run, run)]))
    wait_columns, wait_pair = start_fetches(copies, tiles, tiles_v, sems)
    inv = inv_sqrt_columns(deg_ref)

    def finish(r, total):
        scale = inv[:, r : r + 1]
        hidden = (scale * jax.nn.relu(scale * total + bias_ref[...])).astype(jnp.bfloat16)
        scores = lax.dot_general(wt_ref[...], hidden, NT, preferred_element_type=jnp.float32)
        scores = scores.astype(jnp.bfloat16)
        scores_ref[r] = scores
        table[:, r * blk : (r + 1) * blk] = scores

    def block_sum(r):
        return row_block_sum(
            tiles_v, columns, col_ref, r, lambda left, a, b: jnp.dot(
                left, jnp.concatenate([a, b], axis=0), preferred_element_type=jnp.float32
            )
        )

    wait_columns()
    row_blocks_in_pairs(row_blocks, wait_pair, block_sum, finish)

    def pick(step, carry):
        base = step * 4
        for half in range(2):
            p = base + 2 * half
            slots = jnp.concatenate([send_ref[pl.ds(p, 1)], send_ref[pl.ds(p + 1, 1)]], axis=1)
            picked = jnp.dot(
                table[...], one_hot_cols(slots, rows), preferred_element_type=jnp.float32
            ).astype(out_ref.dtype)
            out_ref[p] = picked[:, :blk]
            out_ref[p + 1] = picked[:, blk:]
        return carry

    lax.fori_loop(0, peers // 4, pick, 0)


def aggregate_inner(
    tile_col, side, left, right, near, far, tiles, deg, bias, w_t, send_lists, groups
):
    classes, hid = w_t.shape
    blocks, blk = deg.shape
    peers = send_lists.shape[0]
    return pl.pallas_call(
        functools.partial(inner_kernel, groups=groups),
        in_specs=[SMEM, SMEM] + [ANY] * 4 + [HBM] + [VMEM] * 4,
        out_specs=[VMEM, VMEM],
        out_shape=[
            jax.ShapeDtypeStruct((blocks, classes, blk), jnp.bfloat16),
            jax.ShapeDtypeStruct((peers, classes, blk), jnp.bfloat16),
        ],
        scratch_shapes=[
            pltpu.VMEM((blocks + peers, blk, hid), jnp.bfloat16),
            pltpu.VMEM(tiles.shape, jnp.bfloat16),
            pltpu.VMEM((classes, blocks * blk), jnp.bfloat16),
            pltpu.SemaphoreType.DMA((2 * blocks + 2 * groups,)),
        ],
        compiler_params=ROOMY,
        name="aggregate_inner",
    )(tile_col, side, left, right, near, far, tiles, deg, bias, w_t, send_lists)


def outer_kernel(
    col_ref, own, arrived, tiles, deg_ref, bias_ref, out_ref, columns, tiles_v, sems
):
    row_blocks, _, blk, _ = tiles.shape
    classes = out_ref.shape[0]
    own_blocks = own.shape[0]
    copies = [
        (own, columns.at[pl.ds(0, own_blocks)]),
        (arrived, columns.at[pl.ds(own_blocks, arrived.shape[0])]),
    ]
    wait_columns, wait_pair = start_fetches(copies, tiles, tiles_v, sems)
    inv = lax.rsqrt(deg_ref[...].astype(jnp.float32))
    square = (classes, classes)
    diagonal = lax.broadcasted_iota(jnp.int32, square, 0) == lax.broadcasted_iota(jnp.int32, square, 1)
    bias = jnp.sum(jnp.where(diagonal, bias_ref[...], 0.0), axis=1, keepdims=True)

    def block_sum(r):
        return row_block_sum(
            tiles_v, columns, col_ref, r, lambda left, a, b: lax.dot_general(
                left, jnp.concatenate([a, b], axis=1), NT, preferred_element_type=jnp.float32
            )
        )

    def finish(r, total):
        out_ref[:, r * blk : (r + 1) * blk] = inv[r : r + 1] * jnp.transpose(total) + bias

    wait_columns()
    row_blocks_in_pairs(row_blocks, wait_pair, block_sum, finish)


def aggregate_outer(tile_col, own, arrived, tiles, deg, bias):
    blocks, classes, blk = own.shape
    peers = arrived.shape[0]
    return pl.pallas_call(
        outer_kernel,
        in_specs=[SMEM, ANY, ANY, HBM, VMEM, VMEM],
        out_specs=VMEM,
        out_shape=jax.ShapeDtypeStruct((classes, blocks * blk), jnp.float32),
        scratch_shapes=[
            pltpu.VMEM((blocks + peers, classes, blk), jnp.bfloat16),
            pltpu.VMEM(tiles.shape, jnp.bfloat16),
            pltpu.SemaphoreType.DMA((2 + blocks,)),
        ],
        compiler_params=ROOMY,
        name="aggregate_outer",
    )(tile_col, own, arrived, tiles, deg, bias)


def exchange(outgoing, axes):
    return lax.all_to_all(outgoing, axes, split_axis=0, concat_axis=0, tiled=True)


def mirror(block):
    return lax.ppermute(block, "hi", [(0, 1), (1, 0)])


def on_device(
    features, w_inner, bias_inner, w_outer, bias_outer, tiles, tile_col, degrees, send_rows, *, groups
):
    near_axes, all_axes = ("dom", "lo"), ("dom", "hi", "lo")
    send_lists = send_rows[0]
    blk = send_lists.shape[1]
    deg = degrees.reshape(-1, blk)
    side = lax.axis_index("hi").reshape(1)
    left, right, near_slots = project(side, features.T, w_inner, deg, send_lists, RIGHT_BLOCKS, groups)
    their_left = mirror(left)
    near_out = pick_near(left, right, near_slots)
    near = exchange(near_out, near_axes)
    their_right = mirror(right)
    part, slots = pick_left(their_left, send_lists.shape[0] // 2, blk)
    far_out = pick_right(part, slots, their_right, deg.size - right.shape[0])
    far = exchange(far_out, near_axes)
    own_scores, outgoing = aggregate_inner(
        tile_col, side, left, right, near, far, tiles, deg,
        bias_inner[None], w_outer.T, send_lists, groups,
    )
    arrived = exchange(outgoing, all_axes)
    return aggregate_outer(tile_col, own_scores, arrived, tiles, deg, bias_outer[None]).T


def solution(mesh):
    groups, inner = mesh.devices.shape
    halves = Mesh(mesh.devices.reshape(groups, 2, inner // 2), ("dom", "hi", "lo"))
    axes = ("dom", "hi", "lo")
    return jax.shard_map(
        functools.partial(on_device, groups=groups),
        mesh=halves,
        in_specs=(
            P(axes, None),
            P(),
            P(),
            P(),
            P(),
            P(axes, None, None, None),
            P(axes, None),
            P(axes),
            P(axes, None, None),
        ),
        out_specs=P(axes, None),
        check_vma=False,
    )
```

```python
import functools

import jax
import jax.numpy as jnp
from jax import lax
from jax.experimental import pallas as pl
from jax.experimental.pallas import tpu as pltpu
from jax.sharding import Mesh
from jax.sharding import PartitionSpec as P

NT = (((1,), (1,)), ((), ()))
TN = (((0,), (0,)), ((), ()))
SMEM = pl.BlockSpec(memory_space=pltpu.SMEM)
VMEM = pl.BlockSpec(memory_space=pltpu.VMEM)
ANY = pl.BlockSpec(memory_space=pl.ANY)
HBM = pl.BlockSpec(memory_space=pltpu.HBM)
ROOMY = pltpu.CompilerParams(vmem_limit_bytes=58 * 2**20)
SMALL = pltpu.CompilerParams(vmem_limit_bytes=24 * 2**20)
LIST_BITS = 5
RIGHT_BLOCKS = 5


def one_hot_rows(slots, rows):
    lane = lax.broadcasted_iota(jnp.int32, (slots.shape[0], rows), 1)
    return jnp.where(slots == lane, 1.0, 0.0).astype(jnp.bfloat16)


def one_hot_cols(slots, rows):
    sub = lax.broadcasted_iota(jnp.int32, (rows, slots.shape[1]), 0)
    return jnp.where(slots == sub, 1.0, 0.0).astype(jnp.bfloat16)


def inv_sqrt_columns(deg_ref):
    return jnp.transpose(lax.rsqrt(deg_ref[...].astype(jnp.float32)))


def half_lists(send_ref, side, groups):
    run = send_ref.shape[0] // (2 * groups)
    runs = []
    for g in range(groups):
        low = send_ref[2 * g * run : (2 * g + 1) * run]
        high = send_ref[(2 * g + 1) * run : (2 * g + 2) * run]
        runs.append(jnp.where(side == 0, low, high))
    return jnp.concatenate(runs, axis=0)


def project_kernel(
    side_ref, feat_ref, w_ref, deg_ref, send_ref, left_ref, right_ref, slots_ref, *, groups
):
    blocks, blk = deg_ref.shape
    left_rows = blocks * blk - right_ref.shape[0]
    inv = inv_sqrt_columns(deg_ref)
    for b in range(blocks):
        part = lax.dot_general(
            feat_ref[:, b * blk : (b + 1) * blk],
            w_ref[...],
            TN,
            preferred_element_type=jnp.float32,
        )
        part = (part * inv[:, b : b + 1]).astype(left_ref.dtype)
        if b * blk < left_rows:
            left_ref[b * blk : (b + 1) * blk, :] = part
        else:
            right_ref[b * blk - left_rows : (b + 1) * blk - left_rows, :] = part
    side = side_ref[0]
    lists = half_lists(send_ref, 1 - side, groups)
    coded = jnp.concatenate([lists >> LIST_BITS, lists & (2**LIST_BITS - 1)], axis=1)
    left_ref[left_rows:, :] = coded.astype(jnp.float32).astype(left_ref.dtype)
    slots_ref[...] = jnp.transpose(half_lists(send_ref, side, groups))


def project(side, feat_t, w_inner, deg, send_lists, right_blocks, groups):
    hid = w_inner.shape[1]
    blocks, blk = deg.shape
    lists = send_lists.shape[0] // 2
    left_rows = (blocks - right_blocks) * blk
    return pl.pallas_call(
        functools.partial(project_kernel, groups=groups),
        in_specs=[SMEM, VMEM, VMEM, VMEM, VMEM],
        out_specs=[VMEM] * 3,
        out_shape=[
            pltpu.VMEM((left_rows + lists, hid), jnp.bfloat16),
            pltpu.VMEM((right_blocks * blk, hid), jnp.bfloat16),
            pltpu.VMEM((blk, lists), jnp.int32),
        ],
        name="project",
    )(side, feat_t, w_inner, deg, send_lists)


def pick_rows(slots, table, first):
    chosen = one_hot_rows(slots - first, table.shape[0])
    return jnp.dot(chosen, table, preferred_element_type=jnp.float32)


def pick_near_kernel(left_ref, right_ref, slots_ref, out_ref):
    lists = out_ref.shape[0]
    left_rows = left_ref.shape[0] - lists
    for p in range(lists):
        column = slots_ref[:, p : p + 1]
        picked = pick_rows(column, left_ref[:left_rows], 0)
        picked = picked + pick_rows(column, right_ref[...], left_rows)
        out_ref[p] = picked.astype(out_ref.dtype)


def pick_near(left, right, slots):
    blk, lists = slots.shape
    return pl.pallas_call(
        pick_near_kernel,
        in_specs=[VMEM, VMEM, VMEM],
        out_specs=VMEM,
        out_shape=pltpu.VMEM((lists, blk, left.shape[1]), jnp.bfloat16),
        compiler_params=SMALL,
        name="pick_near",
    )(left, right, slots)


def pick_left_kernel(left_ref, out_ref, slots_ref):
    lists, blk, _ = out_ref.shape
    left_rows = left_ref.shape[0] - lists
    coded = left_ref[left_rows:].astype(jnp.float32)
    whole = coded[:, :blk] * 2.0**LIST_BITS + coded[:, blk : 2 * blk]
    slots = jnp.transpose(whole).astype(jnp.int32)
    slots_ref[...] = slots
    for p in range(lists):
        picked = pick_rows(slots[:, p : p + 1], left_ref[:left_rows], 0)
        out_ref[p] = picked.astype(out_ref.dtype)


def pick_left(left, lists, blk):
    return pl.pallas_call(
        pick_left_kernel,
        in_specs=[VMEM],
        out_specs=[VMEM, VMEM],
        out_shape=[
            pltpu.VMEM((lists, blk, left.shape[1]), jnp.bfloat16),
            pltpu.VMEM((blk, lists), jnp.int32),
        ],
        compiler_params=SMALL,
        name="pick_left",
    )(left)


def pick_right_kernel(part_ref, slots_ref, right_ref, out_ref, *, left_rows):
    for p in range(out_ref.shape[0]):
        picked = pick_rows(slots_ref[:, p : p + 1], right_ref[...], left_rows)
        out_ref[p] = (part_ref[p].astype(jnp.float32) + picked).astype(out_ref.dtype)


def pick_right(part, slots, right, left_rows):
    return pl.pallas_call(
        functools.partial(pick_right_kernel, left_rows=left_rows),
        in_specs=[VMEM, VMEM, VMEM],
        out_specs=VMEM,
        out_shape=pltpu.VMEM(part.shape, part.dtype),
        compiler_params=SMALL,
        name="pick_right",
    )(part, slots, right)


def start_fetches(column_copies, tiles, tiles_v, sems):
    row_blocks = tiles.shape[0]
    firsts = [
        pltpu.make_async_copy(src, dst, sems.at[row_blocks + i])
        for i, (src, dst) in enumerate(column_copies)
    ]
    sets = [
        pltpu.make_async_copy(tiles.at[r], tiles_v.at[r], sems.at[r]) for r in range(row_blocks)
    ]
    for copy in firsts + sets:
        copy.start()

    def wait_columns():
        for copy in firsts:
            copy.wait()

    def wait_pair(first):
        for copy in sets[first : first + 2]:
            copy.wait()

    return wait_columns, wait_pair


def row_block_sum(tiles_v, columns, col_ref, r, product):
    total = None
    for t in range(0, tiles_v.shape[1], 2):
        left = jnp.concatenate([tiles_v[r, t], tiles_v[r, t + 1]], axis=1)
        part = product(left, columns[col_ref[r, t]], columns[col_ref[r, t + 1]])
        total = part if total is None else total + part
    return total


def row_blocks_in_pairs(row_blocks, wait_pair, pair_sums, finish):
    ready = []
    for first in range(0, row_blocks, 2):
        wait_pair(first)
        sums = pair_sums(first)
        for done in ready:
            finish(*done)
        ready = sums
    for done in ready:
        finish(*done)


def inner_kernel(
    col_ref, side_ref, left, right, near, far, tiles, deg_ref, bias_ref, wt_ref,
    send_ref, scores_ref, out_ref, columns, tiles_v, table, sems, *, groups,
):
    row_blocks, _, blk, _ = tiles.shape
    peers = send_ref.shape[0]
    rows = row_blocks * blk
    run = near.shape[0] // groups
    side = side_ref[0]
    right_blocks = right.shape[0] // blk
    copies = []
    for b in range(row_blocks):
        late = b - (row_blocks - right_blocks)
        source, at = (left, b) if late < 0 else (right, late)
        copies.append((source.at[pl.ds(at * blk, blk)], columns.at[b]))
    for g in range(groups):
        base = row_blocks + 2 * g * run
        group = pl.ds(g * run, run)
        copies.append((near.at[group], columns.at[pl.ds(base + side * run, run)]))
        copies.append((far.at[group], columns.at[pl.ds(base + (1 - side) * run, run)]))
    wait_columns, wait_pair = start_fetches(copies, tiles, tiles_v, sems)
    inv = inv_sqrt_columns(deg_ref)

    def finish(r, total):
        scale = inv[:, r : r + 1]
        hidden = (scale * jax.nn.relu(scale * total + bias_ref[...])).astype(jnp.bfloat16)
        scores = lax.dot_general(wt_ref[...], hidden, NT, preferred_element_type=jnp.float32)
        scores = scores.astype(jnp.bfloat16)
        scores_ref[r] = scores
        table[:, r * blk : (r + 1) * blk] = scores

    def pair_sums(first):
        def product(left, a, b):
            right = jnp.concatenate([a, b], axis=0)
            return jnp.dot(left, right, preferred_element_type=jnp.float32)

        pair = range(first, min(first + 2, row_blocks))
        return [(r, row_block_sum(tiles_v, columns, col_ref, r, product)) for r in pair]

    wait_columns()
    row_blocks_in_pairs(row_blocks, wait_pair, pair_sums, finish)

    def pick(step, carry):
        base = step * 4
        for half in range(2):
            p = base + 2 * half
            slots = jnp.concatenate([send_ref[pl.ds(p, 1)], send_ref[pl.ds(p + 1, 1)]], axis=1)
            picked = jnp.dot(
                table[...], one_hot_cols(slots, rows), preferred_element_type=jnp.float32
            ).astype(out_ref.dtype)
            out_ref[p] = picked[:, :blk]
            out_ref[p + 1] = picked[:, blk:]
        return carry

    lax.fori_loop(0, peers // 4, pick, 0)


def aggregate_inner(
    tile_col, side, left, right, near, far, tiles, deg, bias, w_t, send_lists, groups
):
    classes, hid = w_t.shape
    blocks, blk = deg.shape
    peers = send_lists.shape[0]
    return pl.pallas_call(
        functools.partial(inner_kernel, groups=groups),
        in_specs=[SMEM, SMEM] + [ANY] * 4 + [HBM] + [VMEM] * 4,
        out_specs=[VMEM, VMEM],
        out_shape=[
            pltpu.VMEM((blocks, classes, blk), jnp.bfloat16),
            pltpu.VMEM((peers, classes, blk), jnp.bfloat16),
        ],
        scratch_shapes=[
            pltpu.VMEM((blocks + peers, blk, hid), jnp.bfloat16),
            pltpu.VMEM(tiles.shape, jnp.bfloat16),
            pltpu.VMEM((classes, blocks * blk), jnp.bfloat16),
            pltpu.SemaphoreType.DMA((2 * blocks + 2 * groups,)),
        ],
        compiler_params=ROOMY,
        name="aggregate_inner",
    )(tile_col, side, left, right, near, far, tiles, deg, bias, w_t, send_lists)


def outer_kernel(
    col_ref, own, arrived, tiles, deg_ref, bias_ref, out_ref, columns, tiles_v, sems
):
    row_blocks, per_row, blk, _ = tiles.shape
    classes = out_ref.shape[0]
    own_blocks = own.shape[0]
    copies = [
        (own, columns.at[pl.ds(0, own_blocks)]),
        (arrived, columns.at[pl.ds(own_blocks, arrived.shape[0])]),
    ]
    wait_columns, wait_pair = start_fetches(copies, tiles, tiles_v, sems)
    inv = lax.rsqrt(deg_ref[...].astype(jnp.float32))
    square = (classes, classes)
    diagonal = lax.broadcasted_iota(jnp.int32, square, 0) == lax.broadcasted_iota(jnp.int32, square, 1)
    bias = jnp.sum(jnp.where(diagonal, bias_ref[...], 0.0), axis=1, keepdims=True)

    def pair_sums(first):
        pair = range(first, min(first + 2, row_blocks))
        sums = {r: [None, None] for r in pair}
        for t in range(0, per_row, 4):
            for form in range(2):
                for r in pair:
                    kind = (form + r) % 2
                    u = t + 2 * kind
                    tile = jnp.concatenate([tiles_v[r, u], tiles_v[r, u + 1]], axis=1)
                    block = jnp.concatenate(
                        [columns[col_ref[r, u]], columns[col_ref[r, u + 1]]], axis=1
                    )
                    operands = (block, tile) if kind else (tile, block)
                    part = lax.dot_general(*operands, NT, preferred_element_type=jnp.float32)
                    known = sums[r][kind]
                    sums[r][kind] = part if known is None else known + part
        return list(sums.items())

    def finish(r, sums):
        total = jnp.transpose(sums[0]) + sums[1]
        out_ref[:, r * blk : (r + 1) * blk] = inv[r : r + 1] * total + bias

    wait_columns()
    row_blocks_in_pairs(row_blocks, wait_pair, pair_sums, finish)


def aggregate_outer(tile_col, own, arrived, tiles, deg, bias):
    blocks, classes, blk = own.shape
    peers = arrived.shape[0]
    return pl.pallas_call(
        outer_kernel,
        in_specs=[SMEM, ANY, ANY, HBM, VMEM, VMEM],
        out_specs=VMEM,
        out_shape=jax.ShapeDtypeStruct((classes, blocks * blk), jnp.float32),
        scratch_shapes=[
            pltpu.VMEM((blocks + peers, classes, blk), jnp.bfloat16),
            pltpu.VMEM(tiles.shape, jnp.bfloat16),
            pltpu.SemaphoreType.DMA((2 + blocks,)),
        ],
        compiler_params=ROOMY,
        name="aggregate_outer",
    )(tile_col, own, arrived, tiles, deg, bias)


def exchange(outgoing, axes):
    return lax.all_to_all(outgoing, axes, split_axis=0, concat_axis=0, tiled=True)


def mirror(block):
    return lax.ppermute(block, "hi", [(0, 1), (1, 0)])


def on_device(
    features, w_inner, bias_inner, w_outer, bias_outer, tiles, tile_col, degrees, send_rows, *, groups
):
    near_axes, all_axes = ("dom", "lo"), ("dom", "hi", "lo")
    send_lists = send_rows[0]
    blk = send_lists.shape[1]
    deg = degrees.reshape(-1, blk)
    side = lax.axis_index("hi").reshape(1)
    left, right, near_slots = project(side, features.T, w_inner, deg, send_lists, RIGHT_BLOCKS, groups)
    their_left = mirror(left)
    near_out = pick_near(left, right, near_slots)
    near = exchange(near_out, near_axes)
    their_right = mirror(right)
    part, slots = pick_left(their_left, send_lists.shape[0] // 2, blk)
    far_out = pick_right(part, slots, their_right, deg.size - right.shape[0])
    far = exchange(far_out, near_axes)
    own_scores, outgoing = aggregate_inner(
        tile_col, side, left, right, near, far, tiles, deg,
        bias_inner[None], w_outer.T, send_lists, groups,
    )
    arrived = exchange(outgoing, all_axes)
    return aggregate_outer(tile_col, own_scores, arrived, tiles, deg, bias_outer[None]).T


def solution(mesh):
    groups, inner = mesh.devices.shape
    halves = Mesh(mesh.devices.reshape(groups, 2, inner // 2), ("dom", "hi", "lo"))
    axes = ("dom", "hi", "lo")
    return jax.shard_map(
        functools.partial(on_device, groups=groups),
        mesh=halves,
        in_specs=(
            P(axes, None),
            P(),
            P(),
            P(),
            P(),
            P(axes, None, None, None),
            P(axes, None),
            P(axes),
            P(axes, None, None),
        ),
        out_specs=P(axes, None),
        check_vma=False,
    )
```

```python
import functools

import jax
import jax.numpy as jnp
from jax import lax
from jax.experimental import pallas as pl
from jax.experimental.pallas import tpu as pltpu
from jax.sharding import Mesh
from jax.sharding import PartitionSpec as P

NT = (((1,), (1,)), ((), ()))
TN = (((0,), (0,)), ((), ()))
SMEM = pl.BlockSpec(memory_space=pltpu.SMEM)
VMEM = pl.BlockSpec(memory_space=pltpu.VMEM)
ANY = pl.BlockSpec(memory_space=pl.ANY)
HBM = pl.BlockSpec(memory_space=pltpu.HBM)
ROOMY = pltpu.CompilerParams(vmem_limit_bytes=58 * 2**20)
SMALL = pltpu.CompilerParams(vmem_limit_bytes=24 * 2**20)
LIST_BITS = 5
RIGHT_BLOCKS = 5


def one_hot_rows(slots, rows):
    lane = lax.broadcasted_iota(jnp.int32, (slots.shape[0], rows), 1)
    return jnp.where(slots == lane, 1.0, 0.0).astype(jnp.bfloat16)


def one_hot_cols(slots, rows):
    sub = lax.broadcasted_iota(jnp.int32, (rows, slots.shape[1]), 0)
    return jnp.where(slots == sub, 1.0, 0.0).astype(jnp.bfloat16)


def inv_sqrt_columns(deg_ref):
    return jnp.transpose(lax.rsqrt(deg_ref[...].astype(jnp.float32)))


def half_lists(send_ref, side, groups):
    run = send_ref.shape[0] // (2 * groups)
    runs = []
    for g in range(groups):
        low = send_ref[2 * g * run : (2 * g + 1) * run]
        high = send_ref[(2 * g + 1) * run : (2 * g + 2) * run]
        runs.append(jnp.where(side == 0, low, high))
    return jnp.concatenate(runs, axis=0)


def project_kernel(
    side_ref, feat_ref, w_ref, deg_ref, send_ref, left_ref, right_ref, slots_ref, *, groups
):
    blocks, blk = deg_ref.shape
    left_rows = blocks * blk - right_ref.shape[0]
    inv = inv_sqrt_columns(deg_ref)
    for b in range(blocks):
        part = lax.dot_general(
            feat_ref[:, b * blk : (b + 1) * blk],
            w_ref[...],
            TN,
            preferred_element_type=jnp.float32,
        )
        part = (part * inv[:, b : b + 1]).astype(left_ref.dtype)
        if b * blk < left_rows:
            left_ref[b * blk : (b + 1) * blk, :] = part
        else:
            right_ref[b * blk - left_rows : (b + 1) * blk - left_rows, :] = part
    side = side_ref[0]
    lists = half_lists(send_ref, 1 - side, groups)
    coded = jnp.concatenate([lists >> LIST_BITS, lists & (2**LIST_BITS - 1)], axis=1)
    left_ref[left_rows:, :] = coded.astype(jnp.float32).astype(left_ref.dtype)
    slots_ref[...] = jnp.transpose(half_lists(send_ref, side, groups))


def project(side, feat_t, w_inner, deg, send_lists, right_blocks, groups):
    hid = w_inner.shape[1]
    blocks, blk = deg.shape
    lists = send_lists.shape[0] // 2
    left_rows = (blocks - right_blocks) * blk
    return pl.pallas_call(
        functools.partial(project_kernel, groups=groups),
        in_specs=[SMEM, VMEM, VMEM, VMEM, VMEM],
        out_specs=[VMEM] * 3,
        out_shape=[
            pltpu.VMEM((left_rows + lists, hid), jnp.bfloat16),
            pltpu.VMEM((right_blocks * blk, hid), jnp.bfloat16),
            pltpu.VMEM((blk, lists), jnp.int32),
        ],
        name="project",
    )(side, feat_t, w_inner, deg, send_lists)


def pick_rows(slots, table, first):
    chosen = one_hot_rows(slots - first, table.shape[0])
    return jnp.dot(chosen, table, preferred_element_type=jnp.float32)


def pick_near_kernel(left_ref, right_ref, slots_ref, out_ref):
    lists = out_ref.shape[0]
    left_rows = left_ref.shape[0] - lists
    table = jnp.concatenate([left_ref[:left_rows], right_ref[...]], axis=0)
    for p in range(lists):
        picked = pick_rows(slots_ref[:, p : p + 1], table, 0)
        out_ref[p] = picked.astype(out_ref.dtype)


def pick_near(left, right, slots):
    blk, lists = slots.shape
    return pl.pallas_call(
        pick_near_kernel,
        in_specs=[VMEM, VMEM, VMEM],
        out_specs=VMEM,
        out_shape=pltpu.VMEM((lists, blk, left.shape[1]), jnp.bfloat16),
        compiler_params=SMALL,
        name="pick_near",
    )(left, right, slots)


def pick_left_kernel(left_ref, out_ref, slots_ref):
    lists, blk, _ = out_ref.shape
    left_rows = left_ref.shape[0] - lists
    coded = left_ref[left_rows:].astype(jnp.float32)
    whole = coded[:, :blk] * 2.0**LIST_BITS + coded[:, blk : 2 * blk]
    slots = jnp.transpose(whole).astype(jnp.int32)
    slots_ref[...] = slots
    for p in range(lists):
        picked = pick_rows(slots[:, p : p + 1], left_ref[:left_rows], 0)
        out_ref[p] = picked.astype(out_ref.dtype)


def pick_left(left, lists, blk):
    return pl.pallas_call(
        pick_left_kernel,
        in_specs=[VMEM],
        out_specs=[VMEM, VMEM],
        out_shape=[
            pltpu.VMEM((lists, blk, left.shape[1]), jnp.bfloat16),
            pltpu.VMEM((blk, lists), jnp.int32),
        ],
        compiler_params=SMALL,
        name="pick_left",
    )(left)


def pick_right_kernel(part_ref, slots_ref, right_ref, out_ref, *, left_rows):
    for p in range(out_ref.shape[0]):
        picked = pick_rows(slots_ref[:, p : p + 1], right_ref[...], left_rows)
        out_ref[p] = (part_ref[p].astype(jnp.float32) + picked).astype(out_ref.dtype)


def pick_right(part, slots, right, left_rows):
    return pl.pallas_call(
        functools.partial(pick_right_kernel, left_rows=left_rows),
        in_specs=[VMEM, VMEM, VMEM],
        out_specs=VMEM,
        out_shape=pltpu.VMEM(part.shape, part.dtype),
        compiler_params=SMALL,
        name="pick_right",
    )(part, slots, right)


def start_fetches(column_copies, tiles, tiles_v, sems):
    row_blocks = tiles.shape[0]
    firsts = [
        pltpu.make_async_copy(src, dst, sems.at[row_blocks + i])
        for i, (src, dst) in enumerate(column_copies)
    ]
    sets = [
        pltpu.make_async_copy(tiles.at[r], tiles_v.at[r], sems.at[r]) for r in range(row_blocks)
    ]
    for copy in firsts + sets:
        copy.start()

    def wait_columns():
        for copy in firsts:
            copy.wait()

    def wait_pair(first):
        for copy in sets[first : first + 2]:
            copy.wait()

    return wait_columns, wait_pair


def row_block_sum(tiles_v, columns, col_ref, r, product):
    total = None
    for t in range(0, tiles_v.shape[1], 2):
        left = jnp.concatenate([tiles_v[r, t], tiles_v[r, t + 1]], axis=1)
        part = product(left, columns[col_ref[r, t]], columns[col_ref[r, t + 1]])
        total = part if total is None else total + part
    return total


def row_blocks_in_pairs(row_blocks, wait_pair, pair_sums, finish):
    ready = []
    for first in range(0, row_blocks, 2):
        wait_pair(first)
        sums = pair_sums(first)
        for done in ready:
            finish(*done)
        ready = sums
    for done in ready:
        finish(*done)


def inner_kernel(
    col_ref, side_ref, left, right, near, far, tiles, deg_ref, bias_ref, wt_ref,
    send_ref, scores_ref, out_ref, columns, tiles_v, table, sems, *, groups,
):
    row_blocks, _, blk, _ = tiles.shape
    peers = send_ref.shape[0]
    rows = row_blocks * blk
    run = near.shape[0] // groups
    side = side_ref[0]
    right_blocks = right.shape[0] // blk
    copies = []
    for b in range(row_blocks):
        late = b - (row_blocks - right_blocks)
        source, at = (left, b) if late < 0 else (right, late)
        copies.append((source.at[pl.ds(at * blk, blk)], columns.at[b]))
    for g in range(groups):
        base = row_blocks + 2 * g * run
        group = pl.ds(g * run, run)
        copies.append((near.at[group], columns.at[pl.ds(base + side * run, run)]))
        copies.append((far.at[group], columns.at[pl.ds(base + (1 - side) * run, run)]))
    wait_columns, wait_pair = start_fetches(copies, tiles, tiles_v, sems)
    inv = inv_sqrt_columns(deg_ref)

    def finish(r, total):
        scale = inv[:, r : r + 1]
        hidden = (scale * jax.nn.relu(scale * total + bias_ref[...])).astype(jnp.bfloat16)
        scores = lax.dot_general(wt_ref[...], hidden, NT, preferred_element_type=jnp.float32)
        scores = scores.astype(jnp.bfloat16)
        scores_ref[r] = scores
        table[:, r * blk : (r + 1) * blk] = scores

    def pair_sums(first):
        def product(left, a, b):
            right = jnp.concatenate([a, b], axis=0)
            return jnp.dot(left, right, preferred_element_type=jnp.float32)

        pair = range(first, min(first + 2, row_blocks))
        return [(r, row_block_sum(tiles_v, columns, col_ref, r, product)) for r in pair]

    wait_columns()
    row_blocks_in_pairs(row_blocks, wait_pair, pair_sums, finish)

    def pick(step, carry):
        base = step * 4
        for half in range(2):
            p = base + 2 * half
            slots = jnp.concatenate([send_ref[pl.ds(p, 1)], send_ref[pl.ds(p + 1, 1)]], axis=1)
            picked = jnp.dot(
                table[...], one_hot_cols(slots, rows), preferred_element_type=jnp.float32
            ).astype(out_ref.dtype)
            out_ref[p] = picked[:, :blk]
            out_ref[p + 1] = picked[:, blk:]
        return carry

    lax.fori_loop(0, peers // 4, pick, 0, unroll=8)


def aggregate_inner(
    tile_col, side, left, right, near, far, tiles, deg, bias, w_t, send_lists, groups
):
    classes, hid = w_t.shape
    blocks, blk = deg.shape
    peers = send_lists.shape[0]
    return pl.pallas_call(
        functools.partial(inner_kernel, groups=groups),
        in_specs=[SMEM, SMEM] + [ANY] * 4 + [HBM] + [VMEM] * 4,
        out_specs=[VMEM, VMEM],
        out_shape=[
            pltpu.VMEM((blocks, classes, blk), jnp.bfloat16),
            pltpu.VMEM((peers, classes, blk), jnp.bfloat16),
        ],
        scratch_shapes=[
            pltpu.VMEM((blocks + peers, blk, hid), jnp.bfloat16),
            pltpu.VMEM(tiles.shape, jnp.bfloat16),
            pltpu.VMEM((classes, blocks * blk), jnp.bfloat16),
            pltpu.SemaphoreType.DMA((2 * blocks + 2 * groups,)),
        ],
        compiler_params=ROOMY,
        name="aggregate_inner",
    )(tile_col, side, left, right, near, far, tiles, deg, bias, w_t, send_lists)


def outer_kernel(
    col_ref, own, arrived, tiles, deg_ref, bias_ref, out_ref, columns, tiles_v, sems
):
    row_blocks, per_row, blk, _ = tiles.shape
    classes = out_ref.shape[0]
    own_blocks = own.shape[0]
    copies = [
        (own, columns.at[pl.ds(0, own_blocks)]),
        (arrived, columns.at[pl.ds(own_blocks, arrived.shape[0])]),
    ]
    wait_columns, wait_pair = start_fetches(copies, tiles, tiles_v, sems)
    inv = lax.rsqrt(deg_ref[...].astype(jnp.float32))
    square = (classes, classes)
    diagonal = lax.broadcasted_iota(jnp.int32, square, 0) == lax.broadcasted_iota(jnp.int32, square, 1)
    bias = jnp.sum(jnp.where(diagonal, bias_ref[...], 0.0), axis=1, keepdims=True)

    def pair_sums(first):
        pair = range(first, min(first + 2, row_blocks))
        sums = {r: [None, None] for r in pair}
        for t in range(0, per_row, 4):
            for form in range(2):
                for r in pair:
                    kind = (form + r) % 2
                    u = t + 2 * kind
                    tile = jnp.concatenate([tiles_v[r, u], tiles_v[r, u + 1]], axis=1)
                    block = jnp.concatenate(
                        [columns[col_ref[r, u]], columns[col_ref[r, u + 1]]], axis=1
                    )
                    operands = (block, tile) if kind else (tile, block)
                    part = lax.dot_general(*operands, NT, preferred_element_type=jnp.float32)
                    known = sums[r][kind]
                    sums[r][kind] = part if known is None else known + part
        return list(sums.items())

    def finish(r, sums):
        total = jnp.transpose(sums[0]) + sums[1]
        out_ref[:, r * blk : (r + 1) * blk] = inv[r : r + 1] * total + bias

    wait_columns()
    row_blocks_in_pairs(row_blocks, wait_pair, pair_sums, finish)


def aggregate_outer(tile_col, own, arrived, tiles, deg, bias):
    blocks, classes, blk = own.shape
    peers = arrived.shape[0]
    return pl.pallas_call(
        outer_kernel,
        in_specs=[SMEM, ANY, ANY, HBM, VMEM, VMEM],
        out_specs=VMEM,
        out_shape=jax.ShapeDtypeStruct((classes, blocks * blk), jnp.float32),
        scratch_shapes=[
            pltpu.VMEM((blocks + peers, classes, blk), jnp.bfloat16),
            pltpu.VMEM(tiles.shape, jnp.bfloat16),
            pltpu.SemaphoreType.DMA((2 + blocks,)),
        ],
        compiler_params=ROOMY,
        name="aggregate_outer",
    )(tile_col, own, arrived, tiles, deg, bias)


def exchange(outgoing, axes):
    return lax.all_to_all(outgoing, axes, split_axis=0, concat_axis=0, tiled=True)


def mirror(block):
    return lax.ppermute(block, "hi", [(0, 1), (1, 0)])


def on_device(
    features, w_inner, bias_inner, w_outer, bias_outer, tiles, tile_col, degrees, send_rows, *, groups
):
    near_axes, all_axes = ("dom", "lo"), ("dom", "hi", "lo")
    send_lists = send_rows[0]
    blk = send_lists.shape[1]
    deg = degrees.reshape(-1, blk)
    side = lax.axis_index("hi").reshape(1)
    left, right, near_slots = project(side, features.T, w_inner, deg, send_lists, RIGHT_BLOCKS, groups)
    their_left = mirror(left)
    near_out = pick_near(left, right, near_slots)
    near = exchange(near_out, near_axes)
    their_right = mirror(right)
    part, slots = pick_left(their_left, send_lists.shape[0] // 2, blk)
    far_out = pick_right(part, slots, their_right, deg.size - right.shape[0])
    far = exchange(far_out, near_axes)
    own_scores, outgoing = aggregate_inner(
        tile_col, side, left, right, near, far, tiles, deg,
        bias_inner[None], w_outer.T, send_lists, groups,
    )
    arrived = exchange(outgoing, all_axes)
    return aggregate_outer(tile_col, own_scores, arrived, tiles, deg, bias_outer[None]).T


def solution(mesh):
    groups, inner = mesh.devices.shape
    halves = Mesh(mesh.devices.reshape(groups, 2, inner // 2), ("dom", "hi", "lo"))
    axes = ("dom", "hi", "lo")
    return jax.shard_map(
        functools.partial(on_device, groups=groups),
        mesh=halves,
        in_specs=(
            P(axes, None),
            P(),
            P(),
            P(),
            P(),
            P(axes, None, None, None),
            P(axes, None),
            P(axes),
            P(axes, None, None),
        ),
        out_specs=P(axes, None),
        check_vma=False,
    )
```

```python
import functools

import jax
import jax.numpy as jnp
from jax import lax
from jax.experimental import pallas as pl
from jax.experimental.pallas import tpu as pltpu
from jax.sharding import Mesh
from jax.sharding import PartitionSpec as P

NT = (((1,), (1,)), ((), ()))
TN = (((0,), (0,)), ((), ()))
SMEM = pl.BlockSpec(memory_space=pltpu.SMEM)
VMEM = pl.BlockSpec(memory_space=pltpu.VMEM)
ANY = pl.BlockSpec(memory_space=pl.ANY)
HBM = pl.BlockSpec(memory_space=pltpu.HBM)
ROOMY = pltpu.CompilerParams(vmem_limit_bytes=58 * 2**20)
SMALL = pltpu.CompilerParams(vmem_limit_bytes=24 * 2**20)
LIST_BITS = 5
RIGHT_BLOCKS = 5


def one_hot_rows(slots, rows):
    lane = lax.broadcasted_iota(jnp.int32, (slots.shape[0], rows), 1)
    return jnp.where(slots == lane, 1.0, 0.0).astype(jnp.bfloat16)


def one_hot_cols(slots, rows):
    sub = lax.broadcasted_iota(jnp.int32, (rows, slots.shape[1]), 0)
    return jnp.where(slots == sub, 1.0, 0.0).astype(jnp.bfloat16)


def inv_sqrt_columns(deg_ref):
    return jnp.transpose(lax.rsqrt(deg_ref[...].astype(jnp.float32)))


def half_lists(send_ref, side, groups):
    run = send_ref.shape[0] // (2 * groups)
    runs = []
    for g in range(groups):
        low = send_ref[2 * g * run : (2 * g + 1) * run]
        high = send_ref[(2 * g + 1) * run : (2 * g + 2) * run]
        runs.append(jnp.where(side == 0, low, high))
    return jnp.concatenate(runs, axis=0)


def project_kernel(
    side_ref, feat_ref, w_ref, deg_ref, send_ref, left_ref, right_ref, slots_ref, *, groups
):
    blocks, blk = deg_ref.shape
    left_rows = blocks * blk - right_ref.shape[0]
    inv = inv_sqrt_columns(deg_ref)
    for b in range(blocks):
        part = lax.dot_general(
            feat_ref[:, b * blk : (b + 1) * blk],
            w_ref[...],
            TN,
            preferred_element_type=jnp.float32,
        )
        part = (part * inv[:, b : b + 1]).astype(left_ref.dtype)
        if b * blk < left_rows:
            left_ref[b * blk : (b + 1) * blk, :] = part
        else:
            right_ref[b * blk - left_rows : (b + 1) * blk - left_rows, :] = part
    side = side_ref[0]
    lists = half_lists(send_ref, 1 - side, groups)
    coded = jnp.concatenate([lists >> LIST_BITS, lists & (2**LIST_BITS - 1)], axis=1)
    left_ref[left_rows:, :] = coded.astype(jnp.float32).astype(left_ref.dtype)
    slots_ref[...] = jnp.transpose(half_lists(send_ref, side, groups))


def project(side, feat_t, w_inner, deg, send_lists, right_blocks, groups):
    hid = w_inner.shape[1]
    blocks, blk = deg.shape
    lists = send_lists.shape[0] // 2
    left_rows = (blocks - right_blocks) * blk
    return pl.pallas_call(
        functools.partial(project_kernel, groups=groups),
        in_specs=[SMEM, VMEM, VMEM, VMEM, VMEM],
        out_specs=[VMEM] * 3,
        out_shape=[
            pltpu.VMEM((left_rows + lists, hid), jnp.bfloat16),
            pltpu.VMEM((right_blocks * blk, hid), jnp.bfloat16),
            pltpu.VMEM((blk, lists), jnp.int32),
        ],
        name="project",
    )(side, feat_t, w_inner, deg, send_lists)


def pick_rows(slots, table, first):
    chosen = one_hot_rows(slots - first, table.shape[0])
    return jnp.dot(chosen, table, preferred_element_type=jnp.float32)


def pick_near_kernel(left_ref, right_ref, slots_ref, out, picked_ref, sems):
    lists = picked_ref.shape[0]
    chunk = lists // sems.shape[0]
    left_rows = left_ref.shape[0] - lists
    table = jnp.concatenate([left_ref[:left_rows], right_ref[...]], axis=0)
    copies = []
    for p in range(lists):
        picked = pick_rows(slots_ref[:, p : p + 1], table, 0)
        picked_ref[p] = picked.astype(picked_ref.dtype)
        if (p + 1) % chunk == 0:
            part = pl.ds(p + 1 - chunk, chunk)
            copy = pltpu.make_async_copy(picked_ref.at[part], out.at[part], sems.at[p // chunk])
            copy.start()
            copies.append(copy)
    for copy in copies:
        copy.wait()


def pick_near(left, right, slots):
    blk, lists = slots.shape
    shape = (lists, blk, left.shape[1])
    return pl.pallas_call(
        pick_near_kernel,
        in_specs=[VMEM, VMEM, VMEM],
        out_specs=ANY,
        out_shape=jax.ShapeDtypeStruct(shape, jnp.bfloat16),
        scratch_shapes=[pltpu.VMEM(shape, jnp.bfloat16), pltpu.SemaphoreType.DMA((lists // 4,))],
        compiler_params=SMALL,
        name="pick_near",
    )(left, right, slots)


def pick_left_kernel(left_ref, out_ref, slots_ref):
    lists, blk, _ = out_ref.shape
    left_rows = left_ref.shape[0] - lists
    coded = left_ref[left_rows:].astype(jnp.float32)
    whole = coded[:, :blk] * 2.0**LIST_BITS + coded[:, blk : 2 * blk]
    slots = jnp.transpose(whole).astype(jnp.int32)
    slots_ref[...] = slots
    for p in range(lists):
        picked = pick_rows(slots[:, p : p + 1], left_ref[:left_rows], 0)
        out_ref[p] = picked.astype(out_ref.dtype)


def pick_left(left, lists, blk):
    return pl.pallas_call(
        pick_left_kernel,
        in_specs=[VMEM],
        out_specs=[VMEM, VMEM],
        out_shape=[
            pltpu.VMEM((lists, blk, left.shape[1]), jnp.bfloat16),
            pltpu.VMEM((blk, lists), jnp.int32),
        ],
        compiler_params=SMALL,
        name="pick_left",
    )(left)


def pick_right_kernel(part_ref, slots_ref, right_ref, out_ref, *, left_rows):
    for p in range(out_ref.shape[0]):
        picked = pick_rows(slots_ref[:, p : p + 1], right_ref[...], left_rows)
        out_ref[p] = (part_ref[p].astype(jnp.float32) + picked).astype(out_ref.dtype)


def pick_right(part, slots, right, left_rows):
    return pl.pallas_call(
        functools.partial(pick_right_kernel, left_rows=left_rows),
        in_specs=[VMEM, VMEM, VMEM],
        out_specs=VMEM,
        out_shape=pltpu.VMEM(part.shape, part.dtype),
        compiler_params=SMALL,
        name="pick_right",
    )(part, slots, right)


def start_fetches(column_copies, tiles, tiles_v, sems):
    row_blocks = tiles.shape[0]
    firsts = [
        pltpu.make_async_copy(src, dst, sems.at[row_blocks + i])
        for i, (src, dst) in enumerate(column_copies)
    ]
    sets = [
        pltpu.make_async_copy(tiles.at[r], tiles_v.at[r], sems.at[r]) for r in range(row_blocks)
    ]
    for copy in firsts + sets:
        copy.start()

    def wait_columns():
        for copy in firsts:
            copy.wait()

    def wait_pair(first):
        for copy in sets[first : first + 2]:
            copy.wait()

    return wait_columns, wait_pair


def row_block_sum(tiles_v, columns, col_ref, r, product):
    total = None
    for t in range(0, tiles_v.shape[1], 2):
        left = jnp.concatenate([tiles_v[r, t], tiles_v[r, t + 1]], axis=1)
        part = product(left, columns[col_ref[r, t]], columns[col_ref[r, t + 1]])
        total = part if total is None else total + part
    return total


def row_blocks_in_pairs(row_blocks, wait_pair, pair_sums, finish):
    ready = []
    for first in range(0, row_blocks, 2):
        wait_pair(first)
        sums = pair_sums(first)
        for done in ready:
            finish(*done)
        ready = sums
    for done in ready:
        finish(*done)


def inner_kernel(
    col_ref, side_ref, left, right, near, far, tiles, deg_ref, bias_ref, wt_ref,
    send_ref, scores_ref, out_ref, columns, tiles_v, table, sems, *, groups,
):
    row_blocks, _, blk, _ = tiles.shape
    peers = send_ref.shape[0]
    rows = row_blocks * blk
    run = near.shape[0] // groups
    side = side_ref[0]
    right_blocks = right.shape[0] // blk
    copies = []
    for b in range(row_blocks):
        late = b - (row_blocks - right_blocks)
        source, at = (left, b) if late < 0 else (right, late)
        copies.append((source.at[pl.ds(at * blk, blk)], columns.at[b]))
    for g in range(groups):
        base = row_blocks + 2 * g * run
        group = pl.ds(g * run, run)
        copies.append((near.at[group], columns.at[pl.ds(base + side * run, run)]))
        copies.append((far.at[group], columns.at[pl.ds(base + (1 - side) * run, run)]))
    wait_columns, wait_pair = start_fetches(copies, tiles, tiles_v, sems)
    inv = inv_sqrt_columns(deg_ref)

    def finish(r, total):
        scale = inv[:, r : r + 1]
        hidden = (scale * jax.nn.relu(scale * total + bias_ref[...])).astype(jnp.bfloat16)
        scores = lax.dot_general(wt_ref[...], hidden, NT, preferred_element_type=jnp.float32)
        scores = scores.astype(jnp.bfloat16)
        scores_ref[r] = scores
        table[:, r * blk : (r + 1) * blk] = scores

    def pair_sums(first):
        def product(left, a, b):
            right = jnp.concatenate([a, b], axis=0)
            return jnp.dot(left, right, preferred_element_type=jnp.float32)

        pair = range(first, min(first + 2, row_blocks))
        return [(r, row_block_sum(tiles_v, columns, col_ref, r, product)) for r in pair]

    wait_columns()
    row_blocks_in_pairs(row_blocks, wait_pair, pair_sums, finish)

    def pick(step, carry):
        base = step * 4
        for half in range(2):
            p = base + 2 * half
            slots = jnp.concatenate([send_ref[pl.ds(p, 1)], send_ref[pl.ds(p + 1, 1)]], axis=1)
            picked = jnp.dot(
                table[...], one_hot_cols(slots, rows), preferred_element_type=jnp.float32
            ).astype(out_ref.dtype)
            out_ref[p] = picked[:, :blk]
            out_ref[p + 1] = picked[:, blk:]
        return carry

    lax.fori_loop(0, peers // 4, pick, 0, unroll=8)


def aggregate_inner(
    tile_col, side, left, right, near, far, tiles, deg, bias, w_t, send_lists, groups
):
    classes, hid = w_t.shape
    blocks, blk = deg.shape
    peers = send_lists.shape[0]
    return pl.pallas_call(
        functools.partial(inner_kernel, groups=groups),
        in_specs=[SMEM, SMEM] + [ANY] * 4 + [HBM] + [VMEM] * 4,
        out_specs=[VMEM, VMEM],
        out_shape=[
            pltpu.VMEM((blocks, classes, blk), jnp.bfloat16),
            pltpu.VMEM((peers, classes, blk), jnp.bfloat16),
        ],
        scratch_shapes=[
            pltpu.VMEM((blocks + peers, blk, hid), jnp.bfloat16),
            pltpu.VMEM(tiles.shape, jnp.bfloat16),
            pltpu.VMEM((classes, blocks * blk), jnp.bfloat16),
            pltpu.SemaphoreType.DMA((2 * blocks + 2 * groups,)),
        ],
        compiler_params=ROOMY,
        name="aggregate_inner",
    )(tile_col, side, left, right, near, far, tiles, deg, bias, w_t, send_lists)


def outer_kernel(
    col_ref, own, arrived, tiles, deg_ref, bias_ref, out_ref, columns, tiles_v, sems
):
    row_blocks, per_row, blk, _ = tiles.shape
    classes = out_ref.shape[0]
    own_blocks = own.shape[0]
    copies = [
        (own, columns.at[pl.ds(0, own_blocks)]),
        (arrived, columns.at[pl.ds(own_blocks, arrived.shape[0])]),
    ]
    wait_columns, wait_pair = start_fetches(copies, tiles, tiles_v, sems)
    inv = lax.rsqrt(deg_ref[...].astype(jnp.float32))
    square = (classes, classes)
    diagonal = lax.broadcasted_iota(jnp.int32, square, 0) == lax.broadcasted_iota(jnp.int32, square, 1)
    bias = jnp.sum(jnp.where(diagonal, bias_ref[...], 0.0), axis=1, keepdims=True)

    def pair_sums(first):
        pair = range(first, min(first + 2, row_blocks))
        sums = {r: [None, None] for r in pair}
        for t in range(0, per_row, 4):
            for form in range(2):
                for r in pair:
                    kind = (form + r) % 2
                    u = t + 2 * kind
                    tile = jnp.concatenate([tiles_v[r, u], tiles_v[r, u + 1]], axis=1)
                    block = jnp.concatenate(
                        [columns[col_ref[r, u]], columns[col_ref[r, u + 1]]], axis=1
                    )
                    operands = (block, tile) if kind else (tile, block)
                    part = lax.dot_general(*operands, NT, preferred_element_type=jnp.float32)
                    known = sums[r][kind]
                    sums[r][kind] = part if known is None else known + part
        return list(sums.items())

    def finish(r, sums):
        total = jnp.transpose(sums[0]) + sums[1]
        out_ref[:, r * blk : (r + 1) * blk] = inv[r : r + 1] * total + bias

    wait_columns()
    row_blocks_in_pairs(row_blocks, wait_pair, pair_sums, finish)


def aggregate_outer(tile_col, own, arrived, tiles, deg, bias):
    blocks, classes, blk = own.shape
    peers = arrived.shape[0]
    return pl.pallas_call(
        outer_kernel,
        in_specs=[SMEM, ANY, ANY, HBM, VMEM, VMEM],
        out_specs=VMEM,
        out_shape=jax.ShapeDtypeStruct((classes, blocks * blk), jnp.float32),
        scratch_shapes=[
            pltpu.VMEM((blocks + peers, classes, blk), jnp.bfloat16),
            pltpu.VMEM(tiles.shape, jnp.bfloat16),
            pltpu.SemaphoreType.DMA((2 + blocks,)),
        ],
        compiler_params=ROOMY,
        name="aggregate_outer",
    )(tile_col, own, arrived, tiles, deg, bias)


def exchange(outgoing, axes):
    return lax.all_to_all(outgoing, axes, split_axis=0, concat_axis=0, tiled=True)


def mirror(block):
    return lax.ppermute(block, "hi", [(0, 1), (1, 0)])


def on_device(
    features, w_inner, bias_inner, w_outer, bias_outer, tiles, tile_col, degrees, send_rows, *, groups
):
    near_axes, all_axes = ("dom", "lo"), ("dom", "hi", "lo")
    send_lists = send_rows[0]
    blk = send_lists.shape[1]
    deg = degrees.reshape(-1, blk)
    side = lax.axis_index("hi").reshape(1)
    left, right, near_slots = project(side, features.T, w_inner, deg, send_lists, RIGHT_BLOCKS, groups)
    their_left = mirror(left)
    near_out = pick_near(left, right, near_slots)
    near = exchange(near_out, near_axes)
    their_right = mirror(right)
    part, slots = pick_left(their_left, send_lists.shape[0] // 2, blk)
    far_out = pick_right(part, slots, their_right, deg.size - right.shape[0])
    far = exchange(far_out, near_axes)
    own_scores, outgoing = aggregate_inner(
        tile_col, side, left, right, near, far, tiles, deg,
        bias_inner[None], w_outer.T, send_lists, groups,
    )
    arrived = exchange(outgoing, all_axes)
    return aggregate_outer(tile_col, own_scores, arrived, tiles, deg, bias_outer[None]).T


def solution(mesh):
    groups, inner = mesh.devices.shape
    halves = Mesh(mesh.devices.reshape(groups, 2, inner // 2), ("dom", "hi", "lo"))
    axes = ("dom", "hi", "lo")
    return jax.shard_map(
        functools.partial(on_device, groups=groups),
        mesh=halves,
        in_specs=(
            P(axes, None),
            P(),
            P(),
            P(),
            P(),
            P(axes, None, None, None),
            P(axes, None),
            P(axes),
            P(axes, None, None),
        ),
        out_specs=P(axes, None),
        check_vma=False,
    )
```
